256 devices in a mesh: section: 8 (over y, x_hi), seq: 32 (over z, x_lo, core).
Axes of the slice: x: 4 (x_hi: 2, x_lo: 2; x = x_hi * 2 + x_lo), y: 4, z: 8, core: 2. Of those that a mesh axis runs over, the one named last changes fastest.
Arguments:
- stream: bfloat16 [8, 512, 1536], P('section', 'seq'), may hold values from -6 to 6
- queries: bfloat16 [8, 512, 1536], P('section', 'seq'), may hold values from -40 to 40
- fresh_keys: bfloat16 [8, 512, 1536], P('section', 'seq'), may hold values from -4 to 4
- fresh_values: bfloat16 [8, 512, 1536], P('section', 'seq'), may hold values from -6 to 6
- stale_keys: bfloat16 [8, 4608, 1536], P('section', 'seq'), may hold values from -6 to 6
- stale_values: bfloat16 [8, 4608, 1536], P('section', 'seq'), may hold values from -6 to 6
- gate: float32 [8, 1536], P('section'), may hold values from 0.5 to 4
- patch_of_section: int32 [8], P('section'), may hold values from 0 to 7, as said below
- text_len: int32 [1], replicated, may hold values from 128 to 512
Outputs:
- attended: bfloat16 [8, 512, 1536], P('section', 'seq')
- stream_next: bfloat16 [8, 512, 1536], P('section', 'seq')
The draws below stay inside these ranges and needn't reach their ends.
Inputs may be any that keep to these rules, and one draw needn't show every extreme that they name: `patch_of_section`: section s works on patch (c - s) mod 8 for one c of the draw. The first text_len text positions are used.
All inputs are finite; a program needn't handle non-finite values.
Results may differ from the reference program's by a relative error of at most 0.0085.
Values may be sent and summed in bfloat16 or wider, within the bound.
A program may use at most 64 MiB of HBM per device.

```python
import math
import jax
import jax.numpy as jnp
from jax import lax

HEADS = 12
HDIM = 128
TXT = 512
PATCHES = 8
HW = 1536
PATCH = 512
SEQLEN = 4608
SECTIONS = 8


def joint_draw(key):
    base_key = jax.random.fold_in(key, 7)
    query_seed, key_seed, sign_seed = jax.random.split(base_key, 3)
    full_shape = (SECTIONS, PATCH, HW)
    query_draw = 1.5 * jax.random.truncated_normal(query_seed, -4.0, 4.0, full_shape, jnp.float32)
    key_draw = jax.random.truncated_normal(key_seed, -4.0, 4.0, full_shape, jnp.float32)
    return (query_draw, key_draw)


def draw_queries(key, part):
    return joint_draw(key)[0].astype(jnp.bfloat16)


def draw_fresh_keys(key, part):
    return joint_draw(key)[1].astype(jnp.bfloat16)


def draw_patch_of_section(key, part):
    offset = jax.random.randint(jax.random.fold_in(key, 11), (), 0, PATCHES)
    return ((offset - jnp.arange(SECTIONS, dtype=jnp.int32)) % PATCHES).astype(jnp.int32)


def block_scale(own_key, shape, cuts, low, largest):
    gain = 1.0
    for dim, shards_of in cuts:
        heights = jax.random.uniform(jax.random.fold_in(jax.random.fold_in(own_key, 6), dim), (shards_of,), jnp.float32, low / len(cuts), largest / len(cuts))
        gain = gain * jnp.repeat(jnp.exp(heights), shape[dim] // shards_of).reshape((-1,) + (1,) * (len(shape) - 1 - dim))
    return gain


def scatter_about(key, extent, width, reach, shards=(), kind=jnp.bfloat16):
    loudness = block_scale(key, extent, shards, -0.22, 0.18) if shards else 1.0
    drawn = jax.random.normal(key, extent, jnp.float32) * width * loudness
    return jnp.minimum(jnp.maximum(drawn, -reach), reach).astype(kind)


def setup_inputs(seed: int = 0) -> dict:
    streams_of = jax.random.split(jax.random.key(seed), 10)
    stream = scatter_about(streams_of[0], (SECTIONS, PATCH, HW), 1.0, 6.0, ((0, 8), (1, 32)))
    queries = draw_queries(jax.random.fold_in(streams_of[9], 71), 0)
    fresh_keys = draw_fresh_keys(jax.random.fold_in(streams_of[9], 71), 0)
    fresh_values = scatter_about(streams_of[3], (SECTIONS, PATCH, HW), 1.0, 6.0, ((0, 8), (1, 32)))
    stale_keys = scatter_about(streams_of[4], (SECTIONS, SEQLEN, HW), 1.0, 6.0, ((0, 8), (1, 32)))
    stale_values = scatter_about(streams_of[5], (SECTIONS, SEQLEN, HW), 1.0, 6.0, ((0, 8), (1, 32)))
    gate = jnp.clip(0.5 + 3.5 * jax.random.uniform(streams_of[6], (SECTIONS, HW), jnp.float32) ** block_scale(streams_of[6], (SECTIONS, HW), ((0, 8),), -0.2, 0.2), 0.5, 4.0)
    patch_of_section = draw_patch_of_section(jax.random.fold_in(streams_of[9], 71), 0)
    text_len = jax.random.randint(streams_of[8], (1,), TXT // 4, TXT + 1).astype(jnp.int32)
    return dict(stream=stream, queries=queries, fresh_keys=fresh_keys, fresh_values=fresh_values, stale_keys=stale_keys, stale_values=stale_values, gate=gate, patch_of_section=patch_of_section, text_len=text_len)


def reference(stream, queries, fresh_keys, fresh_values, stale_keys, stale_values, gate, patch_of_section, text_len):
    positions = jnp.arange(SEQLEN, dtype=jnp.int32)
    attended_list = []
    stream_list = []
    for section_index in range(SECTIONS):
        patch_index = patch_of_section[section_index]
        region = (positions - TXT) // PATCH
        stale_ok = jnp.where(positions < TXT, positions < text_len[0], region != patch_index)
        allowed = jnp.concatenate([stale_ok, jnp.ones((PATCH,), dtype=bool)], 0)
        key_block = jnp.concatenate([stale_keys[section_index], fresh_keys[section_index]], 0).astype(jnp.float32).reshape(-1, HEADS, HDIM)
        value_block = jnp.concatenate([stale_values[section_index], fresh_values[section_index]], 0).astype(jnp.float32).reshape(-1, HEADS, HDIM)
        query_block = queries[section_index].astype(jnp.float32).reshape(PATCH, HEADS, HDIM)
        scores = jnp.einsum('qhd,khd->hqk', query_block, key_block) / math.sqrt(HDIM)
        scores = jnp.where(allowed[None, None, :], scores, jnp.float32(-1e+30))
        row_max = lax.optimization_barrier(jnp.max(scores, axis=2))
        weights = jnp.where(allowed[None, None, :], jnp.exp(scores - row_max[:, :, None]), jnp.float32(0.0))
        denominator = lax.optimization_barrier(jnp.sum(weights, axis=2))
        rounded = lax.optimization_barrier(weights.astype(jnp.bfloat16))
        numerator = jnp.einsum('hqk,khd->qhd', rounded.astype(jnp.float32), value_block)
        averaged = numerator / jnp.transpose(denominator)[:, :, None]
        attended_now = averaged.reshape(PATCH, HEADS * HDIM).astype(jnp.bfloat16)
        widened = lax.optimization_barrier(attended_now).astype(jnp.float32)
        incoming = stream[(section_index - 1) % SECTIONS].astype(jnp.float32)
        stream_now = (incoming + gate[section_index][None, :] * widened).astype(jnp.bfloat16)
        attended_list.append(attended_now)
        stream_list.append(stream_now)
    return (jnp.stack(attended_list, 0), jnp.stack(stream_list, 0))
```

```python
import functools
import math

import jax
import jax.numpy as jnp
from jax import lax
from jax.experimental import pallas as pl
from jax.experimental.pallas import tpu as pltpu
from jax.sharding import PartitionSpec as P

HEADS = 12
HDIM = 128
TXT = 512
QUAD = 4
FLOOR_SCORE = -1e30
SCALE = math.log2(math.e) / math.sqrt(HDIM)
MESH = pl.DeviceIdType.MESH


def kernel(
    zs,
    sections,
    stream,
    queries,
    fresh_k,
    fresh_v,
    stale_k,
    stale_v,
    gate,
    patch,
    text,
    att_out,
    next_out,
    q_all,
    k_all,
    v_all,
    part,
    stat,
    got,
    got_stat,
    fin,
    rows_in,
    incoming,
    gate_v,
    next_v,
    local_sem,
    stream_sem,
    q_send,
    q_recv,
    kv_send,
    kv_recv,
    zq_send,
    zq_recv,
    p_send,
    p_recv,
    s_send,
    s_recv,
    f_send,
    f_recv,
):
    section = lax.axis_index("section")
    rank = lax.axis_index("seq")
    z = rank // QUAD
    g = rank % QUAD
    stale = stale_k.shape[0]
    rows = queries.shape[0]
    width = queries.shape[1] // QUAD
    block = rows * QUAD
    heads = width // HDIM

    def quad_peer(k):
        return (g + k) % QUAD

    def z_peer(d):
        return ((z + d) % zs) * QUAD + g

    barrier = pltpu.get_barrier_semaphore()
    peers = [{"seq": z * QUAD + quad_peer(k)} for k in range(1, QUAD)]
    peers += [{"seq": z_peer(d)} for d in range(1, zs)]
    peers += [{"section": (section + 1) % sections}, {"section": (section + sections - 1) % sections}]
    for peer in peers:
        pl.semaphore_signal(barrier, inc=1, device_id=peer, device_id_type=MESH)

    def columns(group):
        return pl.ds(pl.multiple_of(group * width, 128), width)

    def quad_rows(group, count, first=0):
        return pl.ds(pl.multiple_of(first + group * count, 16), count)

    stale_total = stale * QUAD
    sources = (
        (stale_k, k_all, quad_rows(g, stale)),
        (fresh_k, k_all, quad_rows(g, rows, stale_total)),
        (stale_v, v_all, quad_rows(g, stale)),
        (fresh_v, v_all, quad_rows(g, rows, stale_total)),
    )
    mine = columns(g)
    local = [
        pltpu.make_async_copy(queries.at[:, mine], q_all.at[0, quad_rows(g, rows)], local_sem.at[0])
    ]
    for n, (src, dst, where) in enumerate(sources):
        local.append(pltpu.make_async_copy(src.at[:, mine], dst.at[where], local_sem.at[1 + n]))
    local.append(pltpu.make_async_copy(gate, gate_v, local_sem.at[5]))
    for copy in local:
        copy.start()

    pl.semaphore_wait(barrier, len(peers))

    def remote(src, dst, send, recv, peer):
        return pltpu.make_async_remote_copy(
            src_ref=src, dst_ref=dst, send_sem=send, recv_sem=recv, device_id=peer, device_id_type=MESH
        )

    quad_q = []
    for k in range(1, QUAD):
        copy = remote(
            queries.at[:, columns(quad_peer(k))],
            q_all.at[0, quad_rows(g, rows)],
            q_send.at[k - 1],
            q_recv.at[k - 1],
            {"seq": z * QUAD + quad_peer(k)},
        )
        copy.start()
        quad_q.append(copy)
    quad_kv = []
    for n, (src, dst, where) in enumerate(sources):
        for k in range(1, QUAD):
            copy = remote(
                src.at[:, columns(quad_peer(k))],
                dst.at[where],
                kv_send.at[n, k - 1],
                kv_recv.at[n, k - 1],
                {"seq": z * QUAD + quad_peer(k)},
            )
            copy.start()
            quad_kv.append(copy)
    stream_copy = remote(
        stream, incoming, stream_sem.at[0], stream_sem.at[1], {"section": (section + 1) % sections}
    )
    stream_copy.start()

    local[0].wait()
    for copy in quad_q:
        copy.wait_recv()
    order = [d for pair in zip(range(zs // 2, 0, -1), range(zs // 2, zs)) for d in pair]
    order = [d for n, d in enumerate(order) if d not in order[:n]]
    z_q = {}
    for d in order:
        copy = remote(q_all.at[0], q_all.at[d], zq_send.at[d], zq_recv.at[d], {"seq": z_peer(d)})
        copy.start()
        z_q[d] = copy

    spot = lax.broadcasted_iota(jnp.int32, (1, stale_total + block), 1)
    position = z * stale_total + spot
    patch_rows = block * zs
    region = (position - TXT) // patch_rows
    floor = jnp.float32(FLOOR_SCORE)
    text_bias = jnp.where(position < text[0], 0.0, floor)
    image_bias = jnp.where(region == patch[0], floor, 0.0)
    bias = jnp.where(position < TXT, text_bias, image_bias)
    bias = jnp.where(spot < stale_total, bias, 0.0)

    for copy in local[1:]:
        copy.wait()
    for copy in quad_kv:
        copy.wait_recv()

    lane = lax.broadcasted_iota(jnp.int32, (block, 128), 1)
    sent = []
    for d in [0] + order[::-1]:
        if d:
            z_q[d].wait_recv()
        o_ref = got.at[0] if d == 0 else part.at[d]
        s_ref = got_stat.at[0] if d == 0 else stat.at[d]
        stats = jnp.zeros((block, 128), jnp.float32)
        for h in range(heads):
            cols = slice(h * HDIM, (h + 1) * HDIM)
            s = lax.dot_general(
                q_all[d, :, cols],
                k_all[:, cols],
                (((1,), (1,)), ((), ())),
                preferred_element_type=jnp.float32,
            )
            s = s * SCALE + bias
            m = jnp.max(s, axis=1, keepdims=True)
            p = jnp.exp2(s - m)
            total = jnp.sum(p, axis=1, keepdims=True)
            o = jnp.dot(p.astype(jnp.bfloat16), v_all[:, cols], preferred_element_type=jnp.float32)
            o_ref[:, cols] = o.astype(jnp.bfloat16)
            stats = jnp.where(lane == h, m, stats)
            stats = jnp.where(lane == heads + h, total, stats)
        s_ref[:, 0:block] = jnp.transpose(stats)[0:8, :]
        if d:
            peer = {"seq": z_peer(zs - d)}
            for src, dst, send, recv in ((part, got, p_send, p_recv), (stat, got_stat, s_send, s_recv)):
                copy = remote(src.at[d], dst.at[d], send.at[d], recv.at[d], peer)
                copy.start()
                sent.append(copy)

    for copy in sent:
        copy.wait_recv()
    tops = [got_stat[d, 0:heads, 0:block] for d in range(zs)]
    sums = [got_stat[d, heads : 2 * heads, 0:block] for d in range(zs)]
    best = functools.reduce(jnp.maximum, tops)
    factors = [jnp.exp2(t - best) for t in tops]
    whole = functools.reduce(jnp.add, [f * s for f, s in zip(factors, sums)])
    inverse = 1.0 / whole
    rowed = jnp.concatenate([f * inverse for f in factors], axis=0)
    pad = jnp.zeros((128 - heads * zs, block), jnp.float32)
    weight = jnp.transpose(jnp.concatenate([rowed, pad], axis=0))
    for h in range(heads):
        cols = slice(h * HDIM, (h + 1) * HDIM)
        acc = jnp.zeros((block, HDIM), jnp.float32)
        for d in range(zs):
            n = d * heads + h
            acc = acc + weight[:, n : n + 1] * got[d, :, cols].astype(jnp.float32)
        fin[:, cols] = acc.astype(jnp.bfloat16)

    out = []
    for k in range(1, QUAD):
        copy = remote(
            fin.at[quad_rows(quad_peer(k), rows)],
            rows_in.at[g],
            f_send.at[k - 1],
            f_recv.at[k - 1],
            {"seq": z * QUAD + quad_peer(k)},
        )
        copy.start()
        out.append(copy)
    rows_in[g] = fin[quad_rows(g, rows), :]
    stream_copy.wait_recv()
    for copy in out:
        copy.wait_recv()
    for k in range(QUAD):
        cols = slice(k * width, (k + 1) * width)
        att = rows_in[k]
        att_out[:, cols] = att
        next_out[:, cols] = (
            incoming[:, cols].astype(jnp.float32) + gate_v[:, cols] * att.astype(jnp.float32)
        ).astype(jnp.bfloat16)
    for copy in quad_q + quad_kv + [stream_copy] + list(z_q.values()) + sent + out:
        copy.wait_send()


def local(mesh_sizes, stream, queries, fresh_keys, fresh_values, stale_keys, stale_values, gate, patch, text):
    sections, seq = mesh_sizes
    zs = seq // QUAD
    rows, channels = queries.shape[1:]
    stale = stale_keys.shape[1]
    width = channels // QUAD
    block = rows * QUAD
    keys = (stale + rows) * QUAD
    bf16, f32 = jnp.bfloat16, jnp.float32
    dma = pltpu.SemaphoreType.DMA
    hbm = pl.BlockSpec(memory_space=pl.ANY)
    smem = pl.BlockSpec(memory_space=pltpu.SMEM)
    vmem = pl.BlockSpec(memory_space=pltpu.VMEM)
    att, nxt = pl.pallas_call(
        functools.partial(kernel, zs, sections),
        out_shape=[jax.ShapeDtypeStruct((rows, channels), bf16)] * 2,
        in_specs=[hbm] * 7 + [smem] * 2,
        out_specs=[vmem] * 2,
        scratch_shapes=[
            pltpu.VMEM((zs, block, width), bf16),
            pltpu.VMEM((keys, width), bf16),
            pltpu.VMEM((keys, width), bf16),
            pltpu.VMEM((zs, block, width), bf16),
            pltpu.VMEM((zs, 8, 128), f32),
            pltpu.VMEM((zs, block, width), bf16),
            pltpu.VMEM((zs, 8, 128), f32),
            pltpu.VMEM((block, width), bf16),
            pltpu.VMEM((QUAD, rows, width), bf16),
            pltpu.VMEM((rows, channels), bf16),
            pltpu.VMEM((1, channels), f32),
            pltpu.VMEM((rows, channels), bf16),
            dma((6,)),
            dma((2,)),
            dma((3,)),
            dma((3,)),
            dma((4, 3)),
            dma((4, 3)),
            dma((zs,)),
            dma((zs,)),
            dma((zs,)),
            dma((zs,)),
            dma((zs,)),
            dma((zs,)),
            dma((3,)),
            dma((3,)),
        ],
        compiler_params=pltpu.CompilerParams(collective_id=0, has_side_effects=True),
    )(
        stream[0],
        queries[0],
        fresh_keys[0],
        fresh_values[0],
        stale_keys[0],
        stale_values[0],
        gate,
        patch,
        text,
    )
    return att[None], nxt[None]


def solution(mesh):
    rowed = P("section", "seq", None)
    return jax.shard_map(
        functools.partial(local, (mesh.shape["section"], mesh.shape["seq"])),
        mesh=mesh,
        in_specs=(rowed,) * 6 + (P("section", None), P("section"), P()),
        out_specs=(rowed, rowed),
        check_vma=False,
    )
```

```python
import functools
import math

import jax
import jax.numpy as jnp
from jax import lax
from jax.experimental import pallas as pl
from jax.experimental.pallas import tpu as pltpu
from jax.sharding import PartitionSpec as P

HDIM = 128
TXT = 512
QUAD = 4
FLOOR_SCORE = -1e30
SCALE = math.log2(math.e) / math.sqrt(HDIM)
MESH = pl.DeviceIdType.MESH
scope = jax.named_scope


def kernel(
    zs,
    sections,
    stream,
    queries,
    fresh_k,
    fresh_v,
    stale_k,
    stale_v,
    gate,
    patch,
    text,
    att_out,
    next_out,
    q_all,
    k_all,
    v_all,
    part,
    stat,
    got,
    got_stat,
    fin,
    rows_in,
    incoming,
    gate_v,
    patch_s,
    text_s,
    local_sem,
    local_kv,
    stream_sem,
    q_send,
    q_recv,
    kv_send,
    kv_recv,
    zq_send,
    zq_recv,
    p_send,
    p_recv,
    s_send,
    s_recv,
    f_send,
    f_recv,
):
    section = lax.axis_index("section")
    rank = lax.axis_index("seq")
    z = rank // QUAD
    g = rank % QUAD
    stale = stale_k.shape[0]
    rows = queries.shape[0]
    width = queries.shape[1] // QUAD
    block = rows * QUAD
    heads = width // HDIM
    stale_total = stale * QUAD
    after = {"section": (section + 1) % sections}
    before = {"section": (section + sections - 1) % sections}

    def quad_at(k):
        return (g + k) % QUAD

    def quad_peer(k):
        return {"seq": z * QUAD + quad_at(k)}

    def z_peer(d):
        return {"seq": ((z + d + zs) % zs) * QUAD + g}

    barrier = pltpu.get_barrier_semaphore()
    peers = [quad_peer(k) for k in range(1, QUAD)] + [z_peer(d) for d in range(1, zs)] + [after, before]
    for peer in peers:
        pl.semaphore_signal(barrier, inc=1, device_id=peer, device_id_type=MESH)

    def columns(group, head=0, count=width):
        return pl.ds(pl.multiple_of(group * width + head * HDIM, 128), count)

    def quad_rows(group, count, first=0):
        return pl.ds(pl.multiple_of(first + group * count, 16), count)

    sources = (
        (stale_k, k_all, quad_rows(g, stale)),
        (fresh_k, k_all, quad_rows(g, rows, stale_total)),
        (stale_v, v_all, quad_rows(g, stale)),
        (fresh_v, v_all, quad_rows(g, rows, stale_total)),
    )
    small = [
        pltpu.make_async_copy(queries.at[:, columns(g)], q_all.at[0, quad_rows(g, rows)], local_sem.at[0]),
        pltpu.make_async_copy(patch, patch_s, local_sem.at[1]),
        pltpu.make_async_copy(text, text_s, local_sem.at[2]),
        pltpu.make_async_copy(gate, gate_v, local_sem.at[3]),
    ]
    own_kv = [
        [
            pltpu.make_async_copy(src.at[:, columns(g, h, HDIM)], dst.at[h, where], local_kv.at[h, n])
            for n, (src, dst, where) in enumerate(sources)
        ]
        for h in range(heads)
    ]
    for copy in small + sum(own_kv, []):
        copy.start()

    with scope("barrier"):
        pl.semaphore_wait(barrier, len(peers))

    started = []

    def send(src, dst, send_sem, recv_sem, peer):
        copy = pltpu.make_async_remote_copy(
            src_ref=src, dst_ref=dst, send_sem=send_sem, recv_sem=recv_sem, device_id=peer, device_id_type=MESH
        )
        copy.start()
        started.append(copy)
        return copy

    crossing = (2, 3, 1)
    quad_q = [
        send(
            queries.at[:, columns(quad_at(k))],
            q_all.at[0, quad_rows(g, rows)],
            q_send.at[k - 1],
            q_recv.at[k - 1],
            quad_peer(k),
        )
        for k in crossing
    ]
    quad_kv = [
        [
            send(
                src.at[:, columns(quad_at(k), h, HDIM)],
                dst.at[h, where],
                kv_send.at[h, n, k - 1],
                kv_recv.at[h, n, k - 1],
                quad_peer(k),
            )
            for n, (src, dst, where) in enumerate(sources)
            for k in crossing
        ]
        for h in range(heads)
    ]
    stream_copy = send(stream, incoming, stream_sem.at[0], stream_sem.at[1], after)

    with scope("qwait"):
        small[0].wait()
        for copy in quad_q:
            copy.wait_recv()

    arrival = {}

    def pass_on(source, d):
        arrival[d] = [send(q_all.at[source], q_all.at[d], zq_send.at[d], zq_recv.at[d], z_peer(d - source))]

    for d in (2, zs - 2, 1, zs - 1):
        pass_on(0, d)

    with scope("mask"):
        small[1].wait()
        small[2].wait()
        spot = lax.broadcasted_iota(jnp.int32, (1, stale_total + block), 1)
        position = z * stale_total + spot
        region = (position - TXT) // (block * zs)
        floor = jnp.float32(FLOOR_SCORE)
        text_bias = jnp.where(position < text_s[0, 0], 0.0, floor)
        image_bias = jnp.where(region == patch_s[0, 0], floor, 0.0)
        bias = jnp.where(position < TXT, text_bias, image_bias)
        bias = jnp.where(spot < stale_total, bias, 0.0)

    half = block // 2
    with scope("relay"):
        for near, far, turn in ((2, 3, 0), (zs - 2, zs - 3, 1)):
            arrival[near][0].wait_recv()
            pass_on(near, far)
            piece = pl.ds(turn * half, half)
            extra = send(
                q_all.at[near, piece],
                q_all.at[zs // 2, piece],
                zq_send.at[zs // 2 + turn * (zs // 2)],
                zq_recv.at[zs // 2 + turn * (zs // 2)],
                z_peer(near),
            )
            arrival.setdefault(zs // 2, []).append(extra)
    arrival[2], arrival[zs - 2] = [], []
    arrival[0] = []

    lane = lax.broadcasted_iota(jnp.int32, (block, 128), 1)
    partial = [[None] * zs for _ in range(heads)]
    mid = zs // 2
    first_order = [0, 2, zs - 2, 1, zs - 1, 3, zs - 3, mid]
    later_order = [mid, 3, zs - 3, 2, zs - 2, 1, zs - 1, 0]
    for h in range(heads):
        with scope(f"kv#h={h}"):
            for copy in own_kv[h]:
                copy.wait()
            for copy in quad_kv[h]:
                copy.wait_recv()
        cols = slice(h * HDIM, (h + 1) * HDIM)
        stats = jnp.zeros((block, 128), jnp.float32)
        for d in first_order if h == 0 else later_order:
            if h == 0:
                with scope(f"zq#d={d}"):
                    for copy in arrival[d]:
                        copy.wait_recv()
            s = lax.dot_general(
                q_all[d, :, cols], k_all[h], (((1,), (1,)), ((), ())), preferred_element_type=jnp.float32
            )
            s = s * SCALE + bias
            m = jnp.max(s, axis=1, keepdims=True)
            p = jnp.exp2(s - m)
            total = jnp.sum(p, axis=1, keepdims=True)
            o = jnp.dot(p.astype(jnp.bfloat16), v_all[h], preferred_element_type=jnp.float32)
            stats = jnp.where(lane == 2 * d, m, stats)
            stats = jnp.where(lane == 2 * d + 1, total, stats)
            o_ref = part.at[h, d] if d else got.at[h, 0]
            o_ref[...] = o.astype(jnp.bfloat16)
            if d:
                partial[h][d] = send(
                    part.at[h, d], got.at[h, d], p_send.at[h, d], p_recv.at[h, d], z_peer(-d)
                )
        turned = jnp.transpose(stats)
        for d in range(zs):
            s_ref = stat.at[h, d] if d else got_stat.at[h, 0]
            s_ref[:, 0:block] = turned[2 * d : 2 * d + 2, :]
        partial[h] = partial[h][1:] + [
            send(stat.at[h, d], got_stat.at[h, d], s_send.at[h, d], s_recv.at[h, d], z_peer(-d))
            for d in range(1, zs)
        ]

    for h in range(heads):
        with scope(f"pwait#h={h}"):
            for copy in partial[h]:
                copy.wait_recv()
        tops = jnp.concatenate([got_stat[h, d, 0:1, 0:block] for d in range(zs)], axis=0)
        sums = jnp.concatenate([got_stat[h, d, 1:2, 0:block] for d in range(zs)], axis=0)
        factors = jnp.exp2(tops - jnp.max(tops, axis=0, keepdims=True))
        share = factors / jnp.sum(factors * sums, axis=0, keepdims=True)
        pad = jnp.zeros((128 - zs, block), jnp.float32)
        share = jnp.transpose(jnp.concatenate([share, pad], axis=0))
        acc = jnp.zeros((block, HDIM), jnp.float32)
        for d in range(zs):
            acc = acc + share[:, d : d + 1] * got[h, d].astype(jnp.float32)
        fin[:, h * HDIM : (h + 1) * HDIM] = acc.astype(jnp.bfloat16)

    back = [
        send(fin.at[quad_rows(quad_at(k), rows)], rows_in.at[g], f_send.at[k - 1], f_recv.at[k - 1], quad_peer(k))
        for k in crossing
    ]
    rows_in[g] = fin[quad_rows(g, rows), :]
    with scope("owait"):
        small[3].wait()
        stream_copy.wait_recv()
        for copy in back:
            copy.wait_recv()
    for k in range(QUAD):
        cols = slice(k * width, (k + 1) * width)
        att = rows_in[k]
        att_out[:, cols] = att
        next_out[:, cols] = (
            incoming[:, cols].astype(jnp.float32) + gate_v[:, cols] * att.astype(jnp.float32)
        ).astype(jnp.bfloat16)
    with scope("drain"):
        for copy in started:
            copy.wait_send()


def local(mesh_sizes, stream, queries, fresh_keys, fresh_values, stale_keys, stale_values, gate, patch, text):
    sections, seq = mesh_sizes
    zs = seq // QUAD
    rows, channels = queries.shape[1:]
    stale = stale_keys.shape[1]
    width = channels // QUAD
    heads = width // HDIM
    block = rows * QUAD
    keys = (stale + rows) * QUAD
    bf16, f32, i32 = jnp.bfloat16, jnp.float32, jnp.int32
    dma = pltpu.SemaphoreType.DMA
    hbm = pl.BlockSpec(memory_space=pl.ANY)
    vmem = pl.BlockSpec(memory_space=pltpu.VMEM)
    att, nxt = pl.pallas_call(
        functools.partial(kernel, zs, sections),
        out_shape=[pltpu.VMEM((rows, channels), bf16)] * 2,
        in_specs=[hbm] * 9,
        out_specs=[vmem] * 2,
        scratch_shapes=[
            pltpu.VMEM((zs, block, width), bf16),
            pltpu.VMEM((heads, keys, HDIM), bf16),
            pltpu.VMEM((heads, keys, HDIM), bf16),
            pltpu.VMEM((heads, zs, block, HDIM), bf16),
            pltpu.VMEM((heads, zs, 2, 128), f32),
            pltpu.VMEM((heads, zs, block, HDIM), bf16),
            pltpu.VMEM((heads, zs, 2, 128), f32),
            pltpu.VMEM((block, width), bf16),
            pltpu.VMEM((QUAD, rows, width), bf16),
            pltpu.VMEM((rows, channels), bf16),
            pltpu.VMEM((1, channels), f32),
            pltpu.SMEM((1, 1), i32),
            pltpu.SMEM((1, 1), i32),
            dma((4,)),
            dma((heads, 4)),
            dma((2,)),
            dma((3,)),
            dma((3,)),
            dma((heads, 4, 3)),
            dma((heads, 4, 3)),
            dma((zs + 1,)),
            dma((zs + 1,)),
            dma((heads, zs)),
            dma((heads, zs)),
            dma((heads, zs)),
            dma((heads, zs)),
            dma((3,)),
            dma((3,)),
        ],
        compiler_params=pltpu.CompilerParams(
            collective_id=0, has_side_effects=True
        ),
    )(
        stream[0],
        queries[0],
        fresh_keys[0],
        fresh_values[0],
        stale_keys[0],
        stale_values[0],
        gate,
        patch[None],
        text[None],
    )
    return att[None], nxt[None]


def solution(mesh):
    rowed = P("section", "seq", None)
    return jax.shard_map(
        functools.partial(local, (mesh.shape["section"], mesh.shape["seq"])),
        mesh=mesh,
        in_specs=(rowed,) * 6 + (P("section", None), P("section"), P()),
        out_specs=(rowed, rowed),
        check_vma=False,
    )
```

```python
import functools
import math

import jax
import jax.numpy as jnp
from jax import lax
from jax.experimental import pallas as pl
from jax.experimental.pallas import tpu as pltpu
from jax.sharding import PartitionSpec as P

HDIM = 128
TXT = 512
QUAD = 4
FLOOR_SCORE = -1e30
SCALE = math.log2(math.e) / math.sqrt(HDIM)
MESH = pl.DeviceIdType.MESH
scope = jax.named_scope


def kernel(
    zs,
    sections,
    stream,
    queries,
    fresh_k,
    fresh_v,
    stale_k,
    stale_v,
    gate,
    patch,
    text,
    att_out,
    next_out,
    q_all,
    k_all,
    v_all,
    part,
    stat,
    got,
    got_stat,
    fin,
    rows_in,
    incoming,
    gate_v,
    patch_s,
    text_s,
    q_held,
    sk_held,
    fk_held,
    sv_held,
    fv_held,
    local_sem,
    local_kv,
    stream_sem,
    q_send,
    q_recv,
    kv_send,
    kv_recv,
    zq_send,
    zq_recv,
    p_send,
    p_recv,
    s_send,
    s_recv,
    f_send,
    f_recv,
):
    section = lax.axis_index("section")
    rank = lax.axis_index("seq")
    z = rank // QUAD
    g = rank % QUAD
    stale = stale_k.shape[0]
    rows = queries.shape[0]
    width = queries.shape[1] // QUAD
    block = rows * QUAD
    heads = width // HDIM
    stale_total = stale * QUAD
    after = {"section": (section + 1) % sections}
    before = {"section": (section + sections - 1) % sections}

    def quad_at(k):
        return (g + k) % QUAD

    def quad_peer(k):
        return {"seq": z * QUAD + quad_at(k)}

    def z_peer(d):
        return {"seq": ((z + d + zs) % zs) * QUAD + g}

    barrier = pltpu.get_barrier_semaphore()
    peers = [quad_peer(k) for k in range(1, QUAD)] + [z_peer(d) for d in range(1, zs)]
    first = section == 0

    def greet(peer):
        pl.semaphore_signal(barrier, inc=1, device_id=peer, device_id_type=MESH)

    for peer in peers:
        greet(peer)

    @pl.when(section > 1)
    def _():
        greet(before)

    @pl.when(jnp.logical_and(section > 0, section < sections - 1))
    def _():
        greet(after)

    def columns(group, head=0, count=width):
        return pl.ds(pl.multiple_of(group * width + head * HDIM, 128), count)

    def quad_rows(group, count, first=0):
        return pl.ds(pl.multiple_of(first + group * count, 16), count)

    chunk = zs // 2
    order = [0, 1, zs - 1, zs - 2, 2, zs - 3, 3, zs // 2]

    def slot(d, first=0, count=block):
        return pl.ds(pl.multiple_of(order.index(d) * block + first, 16), count)

    sources = (
        (stale_k, k_all, quad_rows(g, stale)),
        (fresh_k, k_all, quad_rows(g, rows, stale_total)),
        (stale_v, v_all, quad_rows(g, stale)),
        (fresh_v, v_all, quad_rows(g, rows, stale_total)),
    )
    small = [
        pltpu.make_async_copy(queries.at[:, columns(g)], q_all.at[slot(0, g * rows, rows)], local_sem.at[0]),
        pltpu.make_async_copy(patch, patch_s, local_sem.at[1]),
        pltpu.make_async_copy(text, text_s, local_sem.at[2]),
        pltpu.make_async_copy(gate, gate_v, local_sem.at[3]),
    ]
    arrays = (stale_k, fresh_k, stale_v, fresh_v)
    staged = [pltpu.make_async_copy(queries, q_held, local_sem.at[4])]
    staged += [
        pltpu.make_async_copy(src, dst, local_sem.at[5 + n])
        for n, (src, dst) in enumerate(zip(arrays, (sk_held, fk_held, sv_held, fv_held)))
    ]
    for copy in staged:
        copy.start()
    own_kv = [
        [
            pltpu.make_async_copy(src.at[:, columns(g, h, HDIM)], dst.at[h, where], local_kv.at[h, n])
            for n, (src, dst, where) in enumerate(sources)
        ]
        for h in range(heads)
    ]
    for copy in small + sum(own_kv, []):
        copy.start()

    with scope("barrier"):

        @pl.when(first)
        def _():
            pl.semaphore_wait(barrier, len(peers))
            greet(after)
            greet(before)

        @pl.when(jnp.logical_not(first))
        def _():
            pl.semaphore_wait(barrier, len(peers) + 2)

        @pl.when(section == 1)
        def _():
            greet(before)

        @pl.when(section == sections - 1)
        def _():
            greet(after)

    started = []

    def send(src, dst, send_sem, recv_sem, peer):
        copy = pltpu.make_async_remote_copy(
            src_ref=src, dst_ref=dst, send_sem=send_sem, recv_sem=recv_sem, device_id=peer, device_id_type=MESH
        )
        copy.start()
        started.append(copy)
        return copy

    crossing = (2, 3, 1)
    for copy in staged:
        copy.wait()
    quad_q = [
        send(
            q_held.at[:, columns(quad_at(k))],
            q_all.at[slot(0, g * rows, rows)],
            q_send.at[k - 1],
            q_recv.at[k - 1],
            quad_peer(k),
        )
        for k in crossing
    ]
    quad_kv = [
        [
            send(
                held.at[:, columns(quad_at(k), h, HDIM)],
                dst.at[h, where],
                kv_send.at[h, n, k - 1],
                kv_recv.at[h, n, k - 1],
                quad_peer(k),
            )
            for n, (held, (_, dst, where)) in enumerate(zip((sk_held, fk_held, sv_held, fv_held), sources))
            for k in crossing
        ]
        for h in range(heads)
    ]

    with scope("qwait"):
        small[0].wait()
        for copy in quad_q:
            copy.wait_recv()

    arrival = {}

    def pass_on(source, d):
        arrival[d] = [send(q_all.at[slot(source)], q_all.at[slot(d)], zq_send.at[d], zq_recv.at[d], z_peer(d - source))]

    for d in (2, zs - 2, 1, zs - 1):
        pass_on(0, d)

    with scope("mask"):
        small[1].wait()
        small[2].wait()
        spot = lax.broadcasted_iota(jnp.int32, (1, stale_total + block), 1)
        position = z * stale_total + spot
        region = (position - TXT) // (block * zs)
        floor = jnp.float32(FLOOR_SCORE)
        text_bias = jnp.where(position < text_s[0, 0], 0.0, floor)
        image_bias = jnp.where(region == patch_s[0, 0], floor, 0.0)
        bias = jnp.where(position < TXT, text_bias, image_bias)
        bias = jnp.where(spot < stale_total, bias, 0.0)

    half = block // 2
    with scope("relay"):
        for near, far, turn in ((2, 3, 0), (zs - 2, zs - 3, 1)):
            arrival[near][0].wait_recv()
            pass_on(near, far)
            extra = send(
                q_all.at[slot(near, turn * half, half)],
                q_all.at[slot(zs // 2, turn * half, half)],
                zq_send.at[zs // 2 + turn * (zs // 2)],
                zq_recv.at[zs // 2 + turn * (zs // 2)],
                z_peer(near),
            )
            arrival.setdefault(zs // 2, []).append(extra)
    arrival[2], arrival[zs - 2] = [], []
    arrival[0] = []

    with scope("greeted"):

        @pl.when(first)
        def _():
            pl.semaphore_wait(barrier, 2)

    stream_copy = send(stream, incoming, stream_sem.at[0], stream_sem.at[1], after)

    lane = lax.broadcasted_iota(jnp.int32, (chunk * block, 128), 1)
    partial = [[] for _ in range(heads)]
    early, late = list(range(chunk)), list(range(chunk, zs))
    for h in range(heads):
        with scope(f"kv#h={h}"):
            for copy in own_kv[h]:
                copy.wait()
            for copy in quad_kv[h]:
                copy.wait_recv()
        cols = slice(h * HDIM, (h + 1) * HDIM)
        for slots in (early, late) if h == 0 else (late, early):
            if h == 0:
                with scope(f"zq#n={slots[0]}"):
                    for n in slots:
                        for copy in arrival[order[n]]:
                            copy.wait_recv()
            s = lax.dot_general(
                q_all[slots[0] * block : slots[0] * block + chunk * block, cols],
                k_all[h],
                (((1,), (1,)), ((), ())),
                preferred_element_type=jnp.float32,
            )
            s = s * SCALE + bias
            m = jnp.max(s, axis=1, keepdims=True)
            p = jnp.exp2(s - m)
            total = jnp.sum(p, axis=1, keepdims=True)
            o = jnp.dot(p.astype(jnp.bfloat16), v_all[h], preferred_element_type=jnp.float32)
            o = o.astype(jnp.bfloat16)
            turned = jnp.transpose(jnp.where(lane == 0, m, total))
            for n in slots if h == 0 else slots[::-1]:
                d = order[n]
                at = slice((n - slots[0]) * block, (n - slots[0] + 1) * block)
                o_ref, s_ref = (part.at[h, d], stat.at[h, d]) if d else (got.at[h, 0], got_stat.at[h, 0])
                o_ref[...] = o[at]
                s_ref[:, 0:block] = turned[0:2, at]
                if d:
                    partial[h].append(
                        send(part.at[h, d], got.at[h, d], p_send.at[h, d], p_recv.at[h, d], z_peer(-d))
                    )
                    partial[h].append(
                        send(stat.at[h, d], got_stat.at[h, d], s_send.at[h, d], s_recv.at[h, d], z_peer(-d))
                    )

    for h in range(heads):
        with scope(f"pwait#h={h}"):
            for copy in partial[h]:
                copy.wait_recv()
        tops = jnp.concatenate([got_stat[h, d, 0:1, 0:block] for d in range(zs)], axis=0)
        sums = jnp.concatenate([got_stat[h, d, 1:2, 0:block] for d in range(zs)], axis=0)
        factors = jnp.exp2(tops - jnp.max(tops, axis=0, keepdims=True))
        share = factors / jnp.sum(factors * sums, axis=0, keepdims=True)
        pad = jnp.zeros((128 - zs, block), jnp.float32)
        share = jnp.transpose(jnp.concatenate([share, pad], axis=0))
        acc = jnp.zeros((block, HDIM), jnp.float32)
        for d in range(zs):
            acc = acc + share[:, d : d + 1] * got[h, d].astype(jnp.float32)
        fin[:, h * HDIM : (h + 1) * HDIM] = acc.astype(jnp.bfloat16)

    back = [
        send(fin.at[quad_rows(quad_at(k), rows)], rows_in.at[g], f_send.at[k - 1], f_recv.at[k - 1], quad_peer(k))
        for k in crossing
    ]
    rows_in[g] = fin[quad_rows(g, rows), :]
    with scope("owait"):
        small[3].wait()
        stream_copy.wait_recv()
        for copy in back:
            copy.wait_recv()
    for k in range(QUAD):
        cols = slice(k * width, (k + 1) * width)
        att = rows_in[k]
        att_out[:, cols] = att
        next_out[:, cols] = (
            incoming[:, cols].astype(jnp.float32) + gate_v[:, cols] * att.astype(jnp.float32)
        ).astype(jnp.bfloat16)
    with scope("drain"):
        for copy in started:
            copy.wait_send()


def local(mesh_sizes, stream, queries, fresh_keys, fresh_values, stale_keys, stale_values, gate, patch, text):
    sections, seq = mesh_sizes
    zs = seq // QUAD
    rows, channels = queries.shape[1:]
    stale = stale_keys.shape[1]
    width = channels // QUAD
    heads = width // HDIM
    block = rows * QUAD
    keys = (stale + rows) * QUAD
    bf16, f32, i32 = jnp.bfloat16, jnp.float32, jnp.int32
    dma = pltpu.SemaphoreType.DMA
    hbm = pl.BlockSpec(memory_space=pl.ANY)
    vmem = pl.BlockSpec(memory_space=pltpu.VMEM)
    att, nxt = pl.pallas_call(
        functools.partial(kernel, zs, sections),
        out_shape=[pltpu.VMEM((rows, channels), bf16)] * 2,
        in_specs=[hbm] * 9,
        out_specs=[vmem] * 2,
        scratch_shapes=[
            pltpu.VMEM((zs * block, width), bf16),
            pltpu.VMEM((heads, keys, HDIM), bf16),
            pltpu.VMEM((heads, keys, HDIM), bf16),
            pltpu.VMEM((heads, zs, block, HDIM), bf16),
            pltpu.VMEM((heads, zs, 2, 128), f32),
            pltpu.VMEM((heads, zs, block, HDIM), bf16),
            pltpu.VMEM((heads, zs, 2, 128), f32),
            pltpu.VMEM((block, width), bf16),
            pltpu.VMEM((QUAD, rows, width), bf16),
            pltpu.VMEM((rows, channels), bf16),
            pltpu.VMEM((1, channels), f32),
            pltpu.SMEM((1, 1), i32),
            pltpu.SMEM((1, 1), i32),
            pltpu.VMEM((rows, channels), bf16),
            pltpu.VMEM((stale, channels), bf16),
            pltpu.VMEM((rows, channels), bf16),
            pltpu.VMEM((stale, channels), bf16),
            pltpu.VMEM((rows, channels), bf16),
            dma((9,)),
            dma((heads, 4)),
            dma((2,)),
            dma((3,)),
            dma((3,)),
            dma((heads, 4, 3)),
            dma((heads, 4, 3)),
            dma((zs + 1,)),
            dma((zs + 1,)),
            dma((heads, zs)),
            dma((heads, zs)),
            dma((heads, zs)),
            dma((heads, zs)),
            dma((3,)),
            dma((3,)),
        ],
        compiler_params=pltpu.CompilerParams(
            collective_id=0, has_side_effects=True
        ),
    )(
        stream[0],
        queries[0],
        fresh_keys[0],
        fresh_values[0],
        stale_keys[0],
        stale_values[0],
        gate,
        patch[None],
        text[None],
    )
    return att[None], nxt[None]


def solution(mesh):
    rowed = P("section", "seq", None)
    return jax.shard_map(
        functools.partial(local, (mesh.shape["section"], mesh.shape["seq"])),
        mesh=mesh,
        in_specs=(rowed,) * 6 + (P("section", None), P("section"), P()),
        out_specs=(rowed, rowed),
        check_vma=False,
    )
```
